512 devices in a mesh: sym: 8 (over y, core), tile: 64 (over z, x).
Axes of the slice: x: 4, y: 4, z: 16, core: 2. Of those that a mesh axis runs over, the one named last changes fastest.
Arguments:
- amplitudes: bfloat16 [256, 131072], P(None, ('sym', 'tile')), may hold values from -6 to 6
- slot_cols: int32 [1024, 64], P(('sym', 'tile')), may hold values from 0 to 127, as said below
- slot_count: int32 [1024], P(('sym', 'tile')), may hold values from 16 to 64, as said below
- integrals: bfloat16 [1024, 64, 128, 128], P(('sym', 'tile')), may hold values from -0.0625 to 0.0625
- cycle_same: bfloat16 [8, 128, 128], P('sym'), may hold values from -0.375 to 0.375
- cycle_cross: bfloat16 [8, 128, 128], P('sym'), may hold values from -0.375 to 0.375
Outputs:
- residual: bfloat16 [256, 131072], P(None, ('sym', 'tile'))
The draws below stay inside these ranges and needn't reach their ends.
Inputs may be any that keep to these rules, and one draw needn't show every extreme that they name: `slot_cols`: tile index within the symmetry block; the live entries of a row are distinct and rising. `slot_count`: some virtual-pair tile has all 64 slots live.
All inputs are finite; a program needn't handle non-finite values.
Results may differ from the reference program's by a relative error of at most 0.0044.
Values may be sent and summed in bfloat16 or wider, within the bound.
A program may use at most 128 MiB of HBM per device.

```python
import jax
import jax.numpy as jnp
from jax import lax

TILE = 128
PAIRS = 256
NTB = 128
SLOTS = 64
NT = 1024
N_SYM = 8


def common_counts(key):
    floor_count = max(1, SLOTS // 4)
    counts = jax.random.randint(jax.random.fold_in(key, 12), (NT,), floor_count, SLOTS + 1, dtype=jnp.int32)
    chosen = jax.random.randint(jax.random.fold_in(key, 13), (), 0, NT, dtype=jnp.int32)
    return jnp.where(jnp.arange(NT, dtype=jnp.int32) == chosen, SLOTS, counts).astype(jnp.int32)


def permute_one(row_key):
    return jax.random.permutation(row_key, NTB)


def draw_slot_cols(key, part):
    counts = common_counts(key)
    row_keys = jax.random.split(jax.random.fold_in(key, 11), NT)
    perms = jax.vmap(permute_one)(row_keys)[:, :SLOTS].astype(jnp.int32)
    live_slot = jnp.arange(SLOTS, dtype=jnp.int32)[None, :] < counts[:, None]
    ordered = jnp.sort(jnp.where(live_slot, perms, perms + NTB), axis=1)
    return jnp.where(ordered >= NTB, ordered - NTB, ordered).astype(jnp.int32)


def draw_slot_count(key, part):
    return common_counts(key)


def shard_levels(rng, shape, shards, low, top_value):
    def one(dim, shards_of):
        heights = jax.random.uniform(jax.random.fold_in(jax.random.fold_in(rng, 6), dim), (shards_of,), jnp.float32, low / len(shards), top_value / len(shards))
        return jnp.repeat(jnp.exp(heights), shape[dim] // shards_of).reshape((-1,) + (1,) * (len(shape) - dim - 1))

    loudness = one(*shards[0])
    for cut in shards[1:]:
        loudness = loudness * one(*cut)
    return loudness


def bell_draw(own_key, shape, scale, bound, shards=(), kind=jnp.bfloat16):
    result = scale * jax.random.normal(own_key, shape, jnp.float32)
    if shards:
        result = result * shard_levels(own_key, shape, shards, -0.22, 0.18)
    return jnp.clip(result, -bound, bound).astype(kind)


def setup_inputs(seed: int = 0) -> dict:
    streams_of = jax.random.split(jax.random.key(seed), 7)
    return {
        "amplitudes": bell_draw(streams_of[0], (PAIRS, NT * TILE), 1.0, 6.0, ((1, 512),)),
        "slot_cols": draw_slot_cols(jax.random.fold_in(streams_of[6], 71), 0),
        "slot_count": draw_slot_count(jax.random.fold_in(streams_of[6], 71), 0),
        "integrals": bell_draw(streams_of[3], (NT, SLOTS, TILE, TILE), (SLOTS * TILE) ** -0.5, 0.0625, ((0, 512),)),
        "cycle_same": bell_draw(streams_of[4], (N_SYM, NTB, NTB), (2 * NTB) ** -0.5, 0.375, ((0, 8),)),
        "cycle_cross": bell_draw(streams_of[5], (N_SYM, NTB, NTB), (2 * NTB) ** -0.5, 0.375, ((0, 8),)),
    }


def reference(amplitudes, slot_cols, slot_count, integrals, cycle_same, cycle_cross):
    pair_count = amplitudes.shape[0]
    amps_four = amplitudes.reshape(pair_count, N_SYM, NTB, TILE)

    def ladder_row(packed):
        tile_id, cols, count, tiles = packed
        block_id = tile_id // NTB
        amp_block = lax.dynamic_index_in_dim(amps_four, block_id, 1, keepdims=False)
        live_slot = jnp.arange(SLOTS, dtype=jnp.int32) < count
        take_index = jnp.where(live_slot, cols, NTB).astype(jnp.int32)
        picked = jnp.take(amp_block, take_index, axis=1, mode="fill", fill_value=0).astype(jnp.float32)
        return jnp.einsum("psc,sac->pa", picked, tiles.astype(jnp.float32))

    ladder_tiles = lax.map(ladder_row, (jnp.arange(NT, dtype=jnp.int32), slot_cols, slot_count, integrals))
    ladder = jnp.transpose(ladder_tiles, (1, 0, 2))
    dressed = (amplitudes.astype(jnp.float32).reshape(pair_count, NT, TILE) + ladder).astype(jnp.bfloat16)
    dressed_four = dressed.reshape(pair_count, N_SYM, NTB, TILE)
    partner = dressed_four.reshape(pair_count, N_SYM // 2, 2, NTB, TILE)[:, :, ::-1].reshape(pair_count, N_SYM, NTB, TILE)
    cycle = jnp.einsum("guv,pgva->pgua", cycle_same.astype(jnp.float32), dressed_four.astype(jnp.float32))
    cycle = cycle + jnp.einsum("guv,pgva->pgua", cycle_cross.astype(jnp.float32), partner.astype(jnp.float32))
    total = ladder + cycle.reshape(pair_count, NT, TILE)
    return total.reshape(pair_count, NT * TILE).astype(jnp.bfloat16)
```

```python
import functools

import jax
import jax.numpy as jnp
from jax import lax
from jax.experimental import pallas as pl
from jax.experimental.pallas import tpu as pltpu
from jax.sharding import PartitionSpec as P

MESH = pl.DeviceIdType.MESH
NX = 4
F32 = jnp.float32
BF16 = jnp.bfloat16


def nt_dot(a, b):
    return lax.dot_general(a, b, (((1,), (1,)), ((), ())), preferred_element_type=F32)


def kernel(
    nz, ra, idx, amps, integ, same, cross, out,
    ga, gb, iv, cv, lm, km, av, acc, acc2, ds, e, rs, r,
    loc, zb_s, zb_r, za_s, za_r, xa_s, xa_r, xb_s, xb_r,
    zd_s, zd_r, xe_s, xe_r, pe_s, pe_r, zr_s, zr_r,
):
    nh = nz // 2
    pairs, width = amps.shape
    rb = pairs - ra
    tw = width // 2
    ps = pairs // nz
    slots = integ.shape[1]
    t = lax.axis_index("tile")
    g = lax.axis_index("sym")
    z, x = t // NX, t % NX
    xl, xr, xo = (x + NX - 1) % NX, (x + 1) % NX, (x + 2) % NX
    xn = (xr, xl)
    zn = ((z + 1) % nz, (z + nz - 1) % nz)
    dev_z = [{"tile": zz * NX + x} for zz in zn]
    dev_x = [{"tile": z * NX + xx} for xx in xn]
    dev_p = {"sym": g + 1 - 2 * (g % 2)}

    def rc(src, dst, ss, rr, dev):
        return pltpu.make_async_remote_copy(
            src_ref=src, dst_ref=dst, send_sem=ss, recv_sem=rr, device_id=dev, device_id_type=MESH
        )

    bar = pltpu.get_barrier_semaphore()
    for dev in dev_z + dev_x + [dev_p]:
        pl.semaphore_signal(bar, inc=1, device_id=dev, device_id_type=MESH)
    pl.semaphore_wait(bar, 5)

    own_a = amps.at[pl.ds(0, ra), :]
    own_b = amps.at[pl.ds(ra, rb), :]
    for d in range(2):
        rc(own_b, gb.at[z, x], zb_s.at[d, 1], zb_r.at[d, 1], dev_z[d]).start()
        rc(own_a, ga.at[z, x], xa_s.at[d], xa_r.at[d], dev_x[d]).start()
    for d in range(2):
        rc(own_b, gb.at[z, x], xb_s.at[0, d], xb_r.at[0, d], dev_x[d]).start()
    local = [
        pltpu.make_async_copy(own_a, ga.at[z, x], loc.at[0]),
        pltpu.make_async_copy(own_b, gb.at[z, x], loc.at[1]),
        pltpu.make_async_copy(amps, av, loc.at[2]),
        pltpu.make_async_copy(same.at[0], cv.at[0], loc.at[3]),
        pltpu.make_async_copy(cross.at[0], cv.at[1], loc.at[4]),
        pltpu.make_async_copy(integ.at[0], iv.at[pl.ds(0, slots)], loc.at[5]),
        pltpu.make_async_copy(integ.at[1], iv.at[pl.ds(slots, slots)], loc.at[6]),
    ]
    for c in local:
        c.start()
    iv[2 * slots] = jnp.zeros((tw, tw), BF16)
    acc[...] = jnp.zeros_like(acc)
    local[0].wait()
    local[1].wait()

    ha, hb = ra // 2, rb // 2

    def half_a(d):
        return pl.ds(d * ha, ha)

    def half_b(d):
        return pl.ds(d * hb, hb)

    def xfrom(d):
        return (xl, xr)[d]

    for d in range(2):
        ref = ga.at[z, xfrom(d)]
        rc(ref, ref, xa_s.at[d], xa_r.at[d], dev_x[d]).wait_recv()
        ref = ga.at[z, xfrom(d), half_a(d), :]
        rc(ref, ref, xa_s.at[2 + d], xa_r.at[2 + d], dev_x[d]).start()
    local[3].wait()
    local[4].wait()
    mrows = lm.shape[1]
    ntb = cv.shape[1]
    row = lax.broadcasted_iota(jnp.int32, (mrows, ntb), 0)
    col = lax.broadcasted_iota(jnp.int32, (mrows, ntb), 1)
    pick = (col == 2 * ((row // (2 * ps)) * NX + x) + (row // ps) % 2).astype(F32).astype(BF16)
    for side in range(2):
        lm[side] = jnp.dot(pick, cv[side], preferred_element_type=F32).astype(BF16)
    for d in range(2):
        ref = ga.at[z, xo, half_a(d), :]
        rc(ref, ref, xa_s.at[2 + d], xa_r.at[2 + d], dev_x[d]).wait_recv()

    def src_z(d, k):
        return (z + nz - k) % nz if d == 0 else (z + k) % nz

    def off(d, k):
        return (nz - k) % nz if d == 0 else k % nz

    def dirs(k):
        return (0,) if (isinstance(k, int) and k in (0, nh)) else (0, 1)

    kcols = nz * ps

    def mix_block(b):
        side, j = b // (2 * NX), b % 2
        xs = (b // 2) % NX
        vv = lax.broadcasted_iota(jnp.int32, (ntb, kcols), 0)
        cc = lax.broadcasted_iota(jnp.int32, (ntb, kcols), 1)
        spread = (vv == 2 * ((cc // ps) * NX + xs) + j).astype(F32).astype(BF16)
        full = jnp.dot(lm[side], spread, preferred_element_type=F32)
        rr = lax.broadcasted_iota(jnp.int32, (mrows, kcols), 0) % ps
        qq = lax.broadcasted_iota(jnp.int32, (mrows, kcols), 1) % ps
        km[b] = jnp.where(rr == qq, full, 0.0).astype(BF16)

    per_step = -(-4 * NX // nh)

    def ladder_terms(s):
        total = acc[...]
        for xs in range(NX):
            base = 2 * (s * NX + xs)
            w = jnp.concatenate(
                [
                    jnp.concatenate([iv[idx[i, base]], iv[idx[i, base + 1]]], axis=1)
                    for i in range(2)
                ],
                axis=0,
            )
            block = jnp.concatenate([ga[s, xs], gb[s, xs]], axis=0)
            total = total + nt_dot(block, w)
        acc[...] = total

    def step(k, first=False, last=False, tail=0):
        if tail == 0:
            for d in range(2):
                s = src_z(d, k)
                ref = gb.at[s, x]
                rc(ref, ref, zb_s.at[d, k], zb_r.at[d, k], dev_z[d]).wait_recv()
                if last:
                    ref = gb.at[s, x, half_b(d), :]
                rc(ref, ref, zb_s.at[d, k + 1], zb_r.at[d, k + 1], dev_z[d]).start()
            sends = (0, 1)
        elif tail == 1:
            s = src_z(0, nh)
            for d in range(2):
                ref = gb.at[s, x, half_b(d), :]
                rc(ref, ref, zb_s.at[d, nh], zb_r.at[d, nh], dev_z[d]).wait_recv()
            sends = (0,)
        else:
            sends = ()
        for side in sends:
            s, o = src_z(side, k), off(side, k)
            for d in range(2):
                ref = gb.at[s, x]
                rc(ref, ref, xb_s.at[o, d], xb_r.at[o, d], dev_x[d]).start()
        if first:
            for d in range(2):
                rc(ga.at[z], ga.at[z], za_s.at[d, 1], za_r.at[d, 1], dev_z[d]).start()
        elif tail <= 1:
            for d in range(2):
                ref = ga.at[src_z(d, k - 1)]
                rc(ref, ref, za_s.at[d, k - 1], za_r.at[d, k - 1], dev_z[d]).wait_recv()
                if tail == 1:
                    ref = ga.at[src_z(d, k - 1), pl.ds(2 * d, 2)]
                rc(ref, ref, za_s.at[d, k], za_r.at[d, k], dev_z[d]).start()
        elif tail == 2:
            for d in range(2):
                ref = ga.at[src_z(0, nh), pl.ds(2 * d, 2)]
                rc(ref, ref, za_s.at[d, nh], za_r.at[d, nh], dev_z[d]).wait_recv()
        if tail <= 2:
            for side in dirs(k - 1):
                s, o = src_z(side, k - 1), off(side, k - 1)
                for d in range(2):
                    ref = gb.at[s, xfrom(d)]
                    rc(ref, ref, xb_s.at[o, d], xb_r.at[o, d], dev_x[d]).wait_recv()
                    ref = gb.at[s, xfrom(d), half_b(d), :]
                    rc(ref, ref, xb_s.at[o, 2 + d], xb_r.at[o, 2 + d], dev_x[d]).start()
        if tail <= 1:
            @pl.loop(0, per_step)
            def _(i):
                b = (k - 1) * per_step + i
                mix_block(b)
        if first:
            for c in local[5:]:
                c.wait()
            return
        for side in dirs(k - 2):
            s, o = src_z(side, k - 2), off(side, k - 2)
            for d in range(2):
                ref = gb.at[s, xo, half_b(d), :]
                rc(ref, ref, xb_s.at[o, 2 + d], xb_r.at[o, 2 + d], dev_x[d]).wait_recv()
            ladder_terms(s)

    step(1, first=True, last=(nh == 2))
    if nh > 2:
        step(2, last=(nh == 3))
        if nh > 4:
            @pl.loop(3, nh - 1)
            def _(k):
                step(k)
        if nh > 3:
            step(nh - 1, last=True)
    for tail in (1, 2, 3):
        step(nh - 1 + tail, tail=tail)

    local[2].wait()
    ds[...] = (av[...].astype(F32) + acc[...]).astype(BF16)

    def order(i):
        return nh + (1 - 2 * (i % 2)) * ((i + 1) // 2)

    def rows_of(zz):
        return pl.ds(pl.multiple_of(zz * ps, ps), ps)

    def z_dev(o):
        return (z + o) % nz, {"tile": ((z + o) % nz) * NX + x}

    @pl.loop(0, nz - 1)
    def _(i):
        o = order(i)
        zz, dev = z_dev(o)
        rc(ds.at[rows_of(zz), :], e.at[0, x, z], zd_s.at[o], zd_r.at[o], dev).start()

    mine = pltpu.make_async_copy(ds.at[rows_of(z), :], e.at[0, x, z], loc.at[0])
    mine.start()
    mine.wait()

    def x_pass(o):
        zs = (z + nz - o) % nz
        for d in range(2):
            ref = e.at[0, x, zs]
            rc(ref, ref, xe_s.at[o, d], xe_r.at[o, d], dev_x[d]).start()

    def x_forward(o):
        zs = (z + nz - o) % nz
        for d in range(2):
            ref = e.at[0, xfrom(d), zs]
            rc(ref, ref, xe_s.at[o, d], xe_r.at[o, d], dev_x[d]).wait_recv()
        sgn = 1 - 2 * (o % 2)
        ref = e.at[0, (x + NX - sgn) % NX, zs]
        dev = {"tile": z * NX + (x + NX + sgn) % NX}
        rc(ref, ref, xe_s.at[o, 2], xe_r.at[o, 2], dev).start()

    x_pass(0)

    @pl.loop(0, nz - 1)
    def _(i):
        o = order(nz - 2 - i)
        zs = (z + nz - o) % nz
        ref = e.at[0, x, zs]
        rc(ref, ref, zd_s.at[o], zd_r.at[o], {"tile": zs * NX + x}).wait_recv()
        x_pass(o)

    def to_partner(dx):
        xs = (x + dx) % NX
        rc(e.at[0, xs], e.at[1, xs], pe_s.at[dx], pe_r.at[dx], dev_p).start()

    def mix(side, dx):
        xs = (x + dx) % NX
        for j in range(2):
            rhs = e[side, xs, :, :, j * tw : (j + 1) * tw].reshape(kcols, tw)
            b = (side * NX + xs) * 2 + j
            acc2[...] += jnp.dot(km[b], rhs, preferred_element_type=F32)

    to_partner(0)
    acc2[...] = jnp.zeros_like(acc2)
    mix(0, 0)
    x_forward(0)

    @pl.loop(0, nz - 1)
    def _(i):
        x_forward(order(nz - 2 - i))

    to_partner(1)
    to_partner(3)
    mix(0, 1)
    mix(0, 3)

    @pl.loop(0, nz)
    def _(o):
        zs = (z + nz - o) % nz
        ref = e.at[0, xo, zs]
        rc(ref, ref, xe_s.at[o, 2], xe_r.at[o, 2], dev_x[0]).wait_recv()

    to_partner(2)
    mix(0, 2)
    for dx in (0, 1, 3, 2):
        xs = (x + dx) % NX
        rc(e.at[0, xs], e.at[1, xs], pe_s.at[dx], pe_r.at[dx], dev_p).wait_recv()
        mix(1, dx)

    rs[...] = acc2[...].astype(BF16).reshape(rs.shape)

    @pl.loop(0, nz - 1)
    def _(i):
        o = order(i)
        zz, dev = z_dev(o)
        rc(rs.at[zz], r.at[z], zr_s.at[o], zr_r.at[o], dev).start()

    r[z] = rs[z]

    def sent(ref, sem):
        rc(ref, ref, sem, sem, dev_p).wait_send()

    for d in range(2):
        sent(own_a, xa_s.at[d])
        sent(ga.at[z, x, half_a(d), :], xa_s.at[2 + d])

        @pl.loop(1, nh)
        def _(k):
            sent(own_b, zb_s.at[d, k])
            sent(ga.at[z], za_s.at[d, k])

        sent(gb.at[z, x, half_b(d), :], zb_s.at[d, nh])
        sent(ga.at[z, pl.ds(0, 2)], za_s.at[d, nh])

    @pl.loop(0, nz)
    def _(o):
        for d in range(2):
            sent(gb.at[z, x], xb_s.at[o, d])
            sent(gb.at[z, x, half_b(d), :], xb_s.at[o, 2 + d])
            sent(e.at[0, x, z], xe_s.at[o, d])
        sent(e.at[0, x, z], xe_s.at[o, 2])

    for dx in range(NX):
        sent(e.at[0, 0], pe_s.at[dx])

    @pl.loop(1, nz)
    def _(o):
        zs = (z + nz - o) % nz
        rc(r.at[zs], r.at[zs], zr_s.at[o], zr_r.at[o], {"tile": zs * NX + x}).wait_recv()
        sent(e.at[0, x, z], zd_s.at[o])
        sent(rs.at[z], zr_s.at[o])

    for j in range(2):
        back = r[:, j].reshape(pairs, tw).astype(F32)
        lanes = slice(j * tw, (j + 1) * tw)
        out[:, lanes] = (acc[:, lanes] + back).astype(BF16)


def on_device(amplitudes, slot_cols, slot_count, integrals, cycle_same, cycle_cross):
    pairs, width = amplitudes.shape
    rows, slots, tw, _ = integrals.shape
    ntb = cycle_same.shape[1]
    nz = lax.axis_size("tile") // NX
    ps = pairs // nz
    ra = (3 * pairs // 8) // 32 * 32
    rb = pairs - ra
    nh = nz // 2
    live = lax.broadcasted_iota(jnp.int32, (rows, slots), 1) < slot_count[:, None]
    cols = jnp.where(live, slot_cols, ntb)
    hit = cols[:, :, None] == lax.broadcasted_iota(jnp.int32, (rows, slots, ntb), 2)
    number = lax.broadcasted_iota(jnp.int32, (rows, slots, ntb), 0) * slots
    number = number + lax.broadcasted_iota(jnp.int32, (rows, slots, ntb), 1)
    idx = jnp.min(jnp.where(hit, number, rows * slots), axis=1)

    dma = pltpu.SemaphoreType.DMA
    anyspace = pl.BlockSpec(memory_space=pl.ANY)
    vm = pltpu.VMEM
    mrows = nz * 2 * ps
    nb = 4 * NX
    per_step = -(-nb // nh)
    return pl.pallas_call(
        functools.partial(kernel, nz, ra),
        out_shape=jax.ShapeDtypeStruct((pairs, width), BF16),
        in_specs=[pl.BlockSpec(memory_space=pltpu.SMEM)] + [anyspace] * 4,
        out_specs=pl.BlockSpec(memory_space=pltpu.VMEM),
        scratch_shapes=[
            vm((nz, NX, ra, width), BF16),
            vm((nz, NX, rb, width), BF16),
            vm((rows * slots + 1, tw, tw), BF16),
            vm((2, ntb, ntb), BF16),
            vm((2, mrows, ntb), BF16),
            vm((per_step * nh, mrows, nz * ps), BF16),
            vm((pairs, width), BF16),
            vm((pairs, width), F32),
            vm((mrows, tw), F32),
            vm((pairs, width), BF16),
            vm((2, NX, nz, ps, width), BF16),
            vm((nz, 2, ps, tw), BF16),
            vm((nz, 2, ps, tw), BF16),
            dma((7,)),
            dma((2, nh + 1)), dma((2, nh + 1)),
            dma((2, nh + 1)), dma((2, nh + 1)),
            dma((4,)), dma((4,)),
            dma((nz, 4)), dma((nz, 4)),
            dma((nz,)), dma((nz,)),
            dma((nz, 3)), dma((nz, 3)),
            dma((NX,)), dma((NX,)),
            dma((nz,)), dma((nz,)),
        ],
        compiler_params=pltpu.CompilerParams(
            collective_id=0, has_side_effects=True, vmem_limit_bytes=48 << 20
        ),
    )(idx, amplitudes, integrals, cycle_same, cycle_cross)


def solution(mesh):
    in_specs = (
        P(None, ("sym", "tile")),
        P(("sym", "tile"), None),
        P(("sym", "tile")),
        P(("sym", "tile"), None, None, None),
        P("sym", None, None),
        P("sym", None, None),
    )
    return jax.shard_map(
        on_device, mesh=mesh, in_specs=in_specs, out_specs=P(None, ("sym", "tile")), check_vma=False
    )
```

```python
import functools

import jax
import jax.numpy as jnp
from jax import lax
from jax.experimental import pallas as pl
from jax.experimental.pallas import tpu as pltpu
from jax.sharding import PartitionSpec as P

MESH = pl.DeviceIdType.MESH
A_LAG = 1
X_LAG = 1
NX = 4
F32 = jnp.float32
BF16 = jnp.bfloat16


def nt_dot(a, b):
    return lax.dot_general(a, b, (((1,), (1,)), ((), ())), preferred_element_type=F32)


def kernel(
    nz, ra, idx, amps, integ, same, cross, out,
    ga, gb, iv, cv, lm, km, av, acc, acc2, ds, e, rs, r,
    loc, zb_s, zb_r, za_s, za_r, xa_s, xa_r, xb_s, xb_r,
    zd_s, zd_r, xe_s, xe_r, pe_s, pe_r, zr_s, zr_r,
):
    nh = nz // 2
    pairs, width = amps.shape
    rb = pairs - ra
    tw = width // 2
    ps = pairs // nz
    slots = integ.shape[1]
    t = lax.axis_index("tile")
    g = lax.axis_index("sym")
    z, x = t // NX, t % NX
    xl, xr, xo = (x + NX - 1) % NX, (x + 1) % NX, (x + 2) % NX
    xn = (xr, xl)
    zn = ((z + 1) % nz, (z + nz - 1) % nz)
    dev_z = [{"tile": zz * NX + x} for zz in zn]
    dev_x = [{"tile": z * NX + xx} for xx in xn]
    dev_p = {"sym": g + 1 - 2 * (g % 2)}

    def rc(src, dst, ss, rr, dev):
        return pltpu.make_async_remote_copy(
            src_ref=src, dst_ref=dst, send_sem=ss, recv_sem=rr, device_id=dev, device_id_type=MESH
        )

    bar = pltpu.get_barrier_semaphore()
    for dev in dev_z + dev_x + [dev_p]:
        pl.semaphore_signal(bar, inc=1, device_id=dev, device_id_type=MESH)
    pl.semaphore_wait(bar, 5)

    own_a = amps.at[pl.ds(0, ra), :]
    own_b = amps.at[pl.ds(ra, rb), :]
    for d in range(2):
        rc(own_b, gb.at[z, x], zb_s.at[d, 1], zb_r.at[d, 1], dev_z[d]).start()
        rc(own_a, ga.at[z, x], xa_s.at[d], xa_r.at[d], dev_x[d]).start()
    for d in range(2):
        rc(own_a, ga.at[z, x], za_s.at[d, 1, 0], za_r.at[d, 1, 0], dev_z[d]).start()
        rc(own_b, gb.at[z, x], xb_s.at[0, d], xb_r.at[0, d], dev_x[d]).start()
    local = [
        pltpu.make_async_copy(own_a, ga.at[z, x], loc.at[0]),
        pltpu.make_async_copy(own_b, gb.at[z, x], loc.at[1]),
        pltpu.make_async_copy(amps, av, loc.at[2]),
        pltpu.make_async_copy(same.at[0], cv.at[0], loc.at[3]),
        pltpu.make_async_copy(cross.at[0], cv.at[1], loc.at[4]),
        pltpu.make_async_copy(integ.at[0], iv.at[pl.ds(0, slots)], loc.at[5]),
        pltpu.make_async_copy(integ.at[1], iv.at[pl.ds(slots, slots)], loc.at[6]),
    ]
    for c in local:
        c.start()
    iv[2 * slots] = jnp.zeros((tw, tw), BF16)
    acc[...] = jnp.zeros_like(acc)

    ha, hb = ra // 2, rb // 2

    def half_a(d):
        return pl.ds(d * ha, ha)

    def half_b(d):
        return pl.ds(d * hb, hb)

    def xfrom(d):
        return (xl, xr)[d]

    parts = (x, xl, xr, xo)
    final = ((0, 3), (1, 2))

    def send_a(d, s, j, k):
        ref = ga.at[s, parts[j]]
        rc(ref, ref, za_s.at[d, k, j], za_r.at[d, k, j], dev_z[d]).start()

    for d in range(2):
        ref = ga.at[z, xfrom(d)]
        rc(ref, ref, xa_s.at[d], xa_r.at[d], dev_x[d]).wait_recv()
        for dz in range(2):
            send_a(dz, z, 1 + d, 1)
        ref = ga.at[z, xfrom(d), half_a(d), :]
        rc(ref, ref, xa_s.at[2 + d], xa_r.at[2 + d], dev_x[d]).start()
    local[3].wait()
    local[4].wait()
    mrows = lm.shape[1]
    ntb = cv.shape[1]
    row = lax.broadcasted_iota(jnp.int32, (mrows, ntb), 0)
    col = lax.broadcasted_iota(jnp.int32, (mrows, ntb), 1)
    pick = (col == 2 * ((row // (2 * ps)) * NX + x) + (row // ps) % 2).astype(F32).astype(BF16)
    for side in range(2):
        lm[side] = jnp.dot(pick, cv[side], preferred_element_type=F32).astype(BF16)
    local[0].wait()
    local[1].wait()

    def src_z(d, k):
        return (z + nz - k) % nz if d == 0 else (z + k) % nz

    def off(d, k):
        return (nz - k) % nz if d == 0 else k % nz

    def dirs(k):
        return (0,) if (isinstance(k, int) and k in (0, nh)) else (0, 1)

    kcols = nz * ps

    def mix_block(b):
        side, j = b // (2 * NX), b % 2
        xs = (b // 2) % NX
        vv = lax.broadcasted_iota(jnp.int32, (ntb, kcols), 0)
        cc = lax.broadcasted_iota(jnp.int32, (ntb, kcols), 1)
        spread = (vv == 2 * ((cc // ps) * NX + xs) + j).astype(F32).astype(BF16)
        full = jnp.dot(lm[side], spread, preferred_element_type=F32)
        rr = lax.broadcasted_iota(jnp.int32, (mrows, kcols), 0) % ps
        qq = lax.broadcasted_iota(jnp.int32, (mrows, kcols), 1) % ps
        km[b] = jnp.where(rr == qq, full, 0.0).astype(BF16)

    per_step = -(-4 * NX // nh)

    def ladder_terms(s):
        total = acc[...]
        for xs in range(NX):
            base = 2 * (s * NX + xs)
            w = jnp.concatenate(
                [
                    jnp.concatenate([iv[idx[i, base]], iv[idx[i, base + 1]]], axis=1)
                    for i in range(2)
                ],
                axis=0,
            )
            block = jnp.concatenate([ga[s, xs], gb[s, xs]], axis=0)
            total = total + nt_dot(block, w)
        acc[...] = total

    def hop_a(k, j, last, ended):
        for d in range(2):
            s = src_z(d, k)
            if ended and j not in final[d]:
                continue
            ref = ga.at[s, parts[j]]
            rc(ref, ref, za_s.at[d, k, j], za_r.at[d, k, j], dev_z[d]).wait_recv()
            if not ended and (not last or j in final[d]):
                send_a(d, s, j, k + 1)

    def step(k):
        inner = not isinstance(k, int)

        def within(v, low, high):
            return inner or low <= v <= high

        if within(k, 1, nh - 1):
            for d in range(2):
                s = src_z(d, k)
                ref = gb.at[s, x]
                rc(ref, ref, zb_s.at[d, k], zb_r.at[d, k], dev_z[d]).wait_recv()
                if not inner and k == nh - 1:
                    ref = gb.at[s, x, half_b(d), :]
                rc(ref, ref, zb_s.at[d, k + 1], zb_r.at[d, k + 1], dev_z[d]).start()
        elif k == nh:
            s = src_z(0, nh)
            for d in range(2):
                ref = gb.at[s, x, half_b(d), :]
                rc(ref, ref, zb_s.at[d, nh], zb_r.at[d, nh], dev_z[d]).wait_recv()
        if within(k, 1, nh):
            for side in dirs(k):
                s, o = src_z(side, k), off(side, k)
                for d in range(2):
                    ref = gb.at[s, x]
                    rc(ref, ref, xb_s.at[o, d], xb_r.at[o, d], dev_x[d]).start()
        kx = k - X_LAG
        if within(kx, 0, nh):
            for side in dirs(kx):
                s, o = src_z(side, kx), off(side, kx)
                for d in range(2):
                    ref = gb.at[s, xfrom(d)]
                    rc(ref, ref, xb_s.at[o, d], xb_r.at[o, d], dev_x[d]).wait_recv()
                    ref = gb.at[s, xfrom(d), half_b(d), :]
                    rc(ref, ref, xb_s.at[o, 2 + d], xb_r.at[o, 2 + d], dev_x[d]).start()
        ka = k - A_LAG
        if within(ka, 1, nh):
            for j in range(3):
                hop_a(ka, j, not inner and ka == nh - 1, not inner and ka == nh)
        ko = k - 1
        if not inner and ko == 0:
            for d in range(2):
                ref = ga.at[z, xo, half_a(d), :]
                rc(ref, ref, xa_s.at[2 + d], xa_r.at[2 + d], dev_x[d]).wait_recv()
            for d in range(2):
                send_a(d, z, 3, 1)
        elif within(ko, 1, nh):
            hop_a(ko, 3, not inner and ko == nh - 1, not inner and ko == nh)
        if within(k, 1, nh):
            @pl.loop(0, per_step)
            def _(i):
                b = (k - 1) * per_step + i
                mix_block(b)
        kl = k - X_LAG - 1
        if not inner and kl == 0:
            for c in local[5:]:
                c.wait()
        if within(kl, 0, nh):
            for side in dirs(kl):
                s, o = src_z(side, kl), off(side, kl)
                for d in range(2):
                    ref = gb.at[s, xo, half_b(d), :]
                    rc(ref, ref, xb_s.at[o, 2 + d], xb_r.at[o, 2 + d], dev_x[d]).wait_recv()
                ladder_terms(s)

    ends = nh + X_LAG + 2
    begin = min(X_LAG + 2, ends)
    stop = max(begin, nh - 1)
    for k in range(1, begin):
        step(k)
    if stop > begin:
        @pl.loop(begin, stop)
        def _(k):
            step(k)
    for k in range(stop, ends):
        step(k)

    local[2].wait()
    ds[...] = (av[...].astype(F32) + acc[...]).astype(BF16)

    def order(i):
        return nh + (1 - 2 * (i % 2)) * ((i + 1) // 2)

    def rows_of(zz):
        return pl.ds(pl.multiple_of(zz * ps, ps), ps)

    def z_dev(o):
        return (z + o) % nz, {"tile": ((z + o) % nz) * NX + x}

    @pl.loop(0, nz - 1)
    def _(i):
        o = order(i)
        zz, dev = z_dev(o)
        rc(ds.at[rows_of(zz), :], e.at[0, x, z], zd_s.at[o], zd_r.at[o], dev).start()

    mine = pltpu.make_async_copy(ds.at[rows_of(z), :], e.at[0, x, z], loc.at[0])
    mine.start()
    mine.wait()

    def x_pass(o):
        zs = (z + nz - o) % nz
        for d in range(2):
            ref = e.at[0, x, zs]
            rc(ref, ref, xe_s.at[o, d], xe_r.at[o, d], dev_x[d]).start()

    def x_forward(o):
        zs = (z + nz - o) % nz
        for d in range(2):
            ref = e.at[0, xfrom(d), zs]
            rc(ref, ref, xe_s.at[o, d], xe_r.at[o, d], dev_x[d]).wait_recv()
        sgn = 1 - 2 * (o % 2)
        ref = e.at[0, (x + NX - sgn) % NX, zs]
        dev = {"tile": z * NX + (x + NX + sgn) % NX}
        rc(ref, ref, xe_s.at[o, 2], xe_r.at[o, 2], dev).start()

    x_pass(0)

    @pl.loop(0, nz - 1)
    def _(i):
        o = order(nz - 2 - i)
        zs = (z + nz - o) % nz
        ref = e.at[0, x, zs]
        rc(ref, ref, zd_s.at[o], zd_r.at[o], {"tile": zs * NX + x}).wait_recv()
        x_pass(o)

    def to_partner(dx):
        xs = (x + dx) % NX
        rc(e.at[0, xs], e.at[1, xs], pe_s.at[dx], pe_r.at[dx], dev_p).start()

    def mix(side, dx):
        xs = (x + dx) % NX
        for j in range(2):
            rhs = e[side, xs, :, :, j * tw : (j + 1) * tw].reshape(kcols, tw)
            b = (side * NX + xs) * 2 + j
            acc2[...] += jnp.dot(km[b], rhs, preferred_element_type=F32)

    to_partner(0)
    acc2[...] = jnp.zeros_like(acc2)
    mix(0, 0)
    x_forward(0)

    @pl.loop(0, nz - 1)
    def _(i):
        x_forward(order(nz - 2 - i))

    to_partner(1)
    to_partner(3)
    mix(0, 1)
    mix(0, 3)

    @pl.loop(0, nz)
    def _(o):
        zs = (z + nz - o) % nz
        ref = e.at[0, xo, zs]
        rc(ref, ref, xe_s.at[o, 2], xe_r.at[o, 2], dev_x[0]).wait_recv()

    to_partner(2)
    mix(0, 2)
    for dx in (0, 1, 3, 2):
        xs = (x + dx) % NX
        rc(e.at[0, xs], e.at[1, xs], pe_s.at[dx], pe_r.at[dx], dev_p).wait_recv()
        mix(1, dx)

    rs[...] = acc2[...].astype(BF16).reshape(rs.shape)

    @pl.loop(0, nz - 1)
    def _(i):
        o = order(i)
        zz, dev = z_dev(o)
        rc(rs.at[zz], r.at[z], zr_s.at[o], zr_r.at[o], dev).start()

    r[z] = rs[z]

    def sent(ref, sem):
        rc(ref, ref, sem, sem, dev_p).wait_send()

    for d in range(2):
        sent(own_a, xa_s.at[d])
        sent(ga.at[z, x, half_a(d), :], xa_s.at[2 + d])

        @pl.loop(1, nh)
        def _(k):
            sent(own_b, zb_s.at[d, k])
            for j in range(NX):
                sent(own_a, za_s.at[d, k, j])

        sent(gb.at[z, x, half_b(d), :], zb_s.at[d, nh])
        for j in final[d]:
            sent(own_a, za_s.at[d, nh, j])

    @pl.loop(0, nz)
    def _(o):
        for d in range(2):
            sent(gb.at[z, x], xb_s.at[o, d])
            sent(gb.at[z, x, half_b(d), :], xb_s.at[o, 2 + d])
            sent(e.at[0, x, z], xe_s.at[o, d])
        sent(e.at[0, x, z], xe_s.at[o, 2])

    for dx in range(NX):
        sent(e.at[0, 0], pe_s.at[dx])

    @pl.loop(1, nz)
    def _(o):
        zs = (z + nz - o) % nz
        rc(r.at[zs], r.at[zs], zr_s.at[o], zr_r.at[o], {"tile": zs * NX + x}).wait_recv()
        sent(e.at[0, x, z], zd_s.at[o])
        sent(rs.at[z], zr_s.at[o])

    for j in range(2):
        back = r[:, j].reshape(pairs, tw).astype(F32)
        lanes = slice(j * tw, (j + 1) * tw)
        out[:, lanes] = (acc[:, lanes] + back).astype(BF16)


def on_device(amplitudes, slot_cols, slot_count, integrals, cycle_same, cycle_cross):
    pairs, width = amplitudes.shape
    rows, slots, tw, _ = integrals.shape
    ntb = cycle_same.shape[1]
    nz = lax.axis_size("tile") // NX
    ps = pairs // nz
    ra = (3 * pairs // 8) // 32 * 32
    rb = pairs - ra
    nh = nz // 2
    live = lax.broadcasted_iota(jnp.int32, (rows, slots), 1) < slot_count[:, None]
    cols = jnp.where(live, slot_cols, ntb)
    hit = cols[:, :, None] == lax.broadcasted_iota(jnp.int32, (rows, slots, ntb), 2)
    number = lax.broadcasted_iota(jnp.int32, (rows, slots, ntb), 0) * slots
    number = number + lax.broadcasted_iota(jnp.int32, (rows, slots, ntb), 1)
    idx = jnp.min(jnp.where(hit, number, rows * slots), axis=1)

    dma = pltpu.SemaphoreType.DMA
    anyspace = pl.BlockSpec(memory_space=pl.ANY)
    vm = pltpu.VMEM
    mrows = nz * 2 * ps
    nb = 4 * NX
    per_step = -(-nb // nh)
    return pl.pallas_call(
        functools.partial(kernel, nz, ra),
        out_shape=jax.ShapeDtypeStruct((pairs, width), BF16),
        in_specs=[pl.BlockSpec(memory_space=pltpu.SMEM)] + [anyspace] * 4,
        out_specs=pl.BlockSpec(memory_space=pltpu.VMEM),
        scratch_shapes=[
            vm((nz, NX, ra, width), BF16),
            vm((nz, NX, rb, width), BF16),
            vm((rows * slots + 1, tw, tw), BF16),
            vm((2, ntb, ntb), BF16),
            vm((2, mrows, ntb), BF16),
            vm((per_step * nh, mrows, nz * ps), BF16),
            vm((pairs, width), BF16),
            vm((pairs, width), F32),
            vm((mrows, tw), F32),
            vm((pairs, width), BF16),
            vm((2, NX, nz, ps, width), BF16),
            vm((nz, 2, ps, tw), BF16),
            vm((nz, 2, ps, tw), BF16),
            dma((7,)),
            dma((2, nh + 1)), dma((2, nh + 1)),
            dma((2, nh + 1, NX)), dma((2, nh + 1, NX)),
            dma((4,)), dma((4,)),
            dma((nz, 4)), dma((nz, 4)),
            dma((nz,)), dma((nz,)),
            dma((nz, 3)), dma((nz, 3)),
            dma((NX,)), dma((NX,)),
            dma((nz,)), dma((nz,)),
        ],
        compiler_params=pltpu.CompilerParams(
            collective_id=0, has_side_effects=True, vmem_limit_bytes=67043328
        ),
    )(idx, amplitudes, integrals, cycle_same, cycle_cross)


def solution(mesh):
    in_specs = (
        P(None, ("sym", "tile")),
        P(("sym", "tile"), None),
        P(("sym", "tile")),
        P(("sym", "tile"), None, None, None),
        P("sym", None, None),
        P("sym", None, None),
    )
    return jax.shard_map(
        on_device, mesh=mesh, in_specs=in_specs, out_specs=P(None, ("sym", "tile")), check_vma=False
    )
```

```python
import functools

import jax
import jax.numpy as jnp
from jax import lax
from jax.experimental import pallas as pl
from jax.experimental.pallas import tpu as pltpu
from jax.sharding import PartitionSpec as P

MESH = pl.DeviceIdType.MESH
A_LAG = 1
X_LAG = 1
NX = 4
F32 = jnp.float32
BF16 = jnp.bfloat16


def nt_dot(a, b):
    return lax.dot_general(a, b, (((1,), (1,)), ((), ())), preferred_element_type=F32)


def kernel(
    nz, ra, idx, amps, integ, same, cross, out,
    ga, gb, iv, cv, lm, km, av, acc, acc2, ds, e, rs, r,
    loc, zb_s, zb_r, za_s, za_r, xa_s, xa_r, xb_s, xb_r,
    zd_s, zd_r, xe_s, xe_r, pe_s, pe_r, zr_s, zr_r,
):
    nh = nz // 2
    pairs, width = amps.shape
    rb = pairs - ra
    tw = width // 2
    ps = pairs // nz
    slots = integ.shape[1]
    t = lax.axis_index("tile")
    g = lax.axis_index("sym")
    z, x = t // NX, t % NX
    xl, xr, xo = (x + NX - 1) % NX, (x + 1) % NX, (x + 2) % NX
    xn = (xr, xl)
    zn = ((z + 1) % nz, (z + nz - 1) % nz)
    dev_z = [{"tile": zz * NX + x} for zz in zn]
    dev_x = [{"tile": z * NX + xx} for xx in xn]
    dev_p = {"sym": g + 1 - 2 * (g % 2)}

    def rc(src, dst, ss, rr, dev):
        return pltpu.make_async_remote_copy(
            src_ref=src, dst_ref=dst, send_sem=ss, recv_sem=rr, device_id=dev, device_id_type=MESH
        )

    bar = pltpu.get_barrier_semaphore()
    for dev in dev_z + dev_x + [dev_p]:
        pl.semaphore_signal(bar, inc=1, device_id=dev, device_id_type=MESH)
    pl.semaphore_wait(bar, 5)

    own_a = amps.at[pl.ds(0, ra), :]
    own_b = amps.at[pl.ds(ra, rb), :]
    for d in range(2):
        rc(own_b, gb.at[z, x], zb_s.at[d, 1], zb_r.at[d, 1], dev_z[d]).start()
        rc(own_a, ga.at[z, x], xa_s.at[d], xa_r.at[d], dev_x[d]).start()
    for d in range(2):
        rc(own_a, ga.at[z, x], za_s.at[d, 1, 0], za_r.at[d, 1, 0], dev_z[d]).start()
        rc(own_b, gb.at[z, x], xb_s.at[0, d], xb_r.at[0, d], dev_x[d]).start()
    local = [
        pltpu.make_async_copy(own_a, ga.at[z, x], loc.at[0]),
        pltpu.make_async_copy(own_b, gb.at[z, x], loc.at[1]),
        pltpu.make_async_copy(amps, av, loc.at[2]),
        pltpu.make_async_copy(same.at[0], cv.at[0], loc.at[3]),
        pltpu.make_async_copy(cross.at[0], cv.at[1], loc.at[4]),
        pltpu.make_async_copy(integ.at[0], iv.at[pl.ds(0, slots)], loc.at[5]),
        pltpu.make_async_copy(integ.at[1], iv.at[pl.ds(slots, slots)], loc.at[6]),
    ]
    for c in local:
        c.start()
    iv[2 * slots] = jnp.zeros((tw, tw), BF16)
    acc[...] = jnp.zeros_like(acc)

    ha, hb = ra // 2, rb // 2

    def half_a(d):
        return pl.ds(d * ha, ha)

    def half_b(d):
        return pl.ds(d * hb, hb)

    def xfrom(d):
        return (xl, xr)[d]

    parts = (x, xl, xr, xo)
    final = ((0, 3), (1, 2))

    def send_a(d, s, j, k):
        ref = ga.at[s, parts[j]]
        rc(ref, ref, za_s.at[d, k, j], za_r.at[d, k, j], dev_z[d]).start()

    for d in range(2):
        ref = ga.at[z, xfrom(d)]
        rc(ref, ref, xa_s.at[d], xa_r.at[d], dev_x[d]).wait_recv()
        for dz in range(2):
            send_a(dz, z, 1 + d, 1)
        ref = ga.at[z, xfrom(d), half_a(d), :]
        rc(ref, ref, xa_s.at[2 + d], xa_r.at[2 + d], dev_x[d]).start()
    local[3].wait()
    local[4].wait()
    mrows = lm.shape[1]
    ntb = cv.shape[1]
    row = lax.broadcasted_iota(jnp.int32, (mrows, ntb), 0)
    col = lax.broadcasted_iota(jnp.int32, (mrows, ntb), 1)
    pick = (col == 2 * ((row // (2 * ps)) * NX + x) + (row // ps) % 2).astype(F32).astype(BF16)
    for side in range(2):
        lm[side] = jnp.dot(pick, cv[side], preferred_element_type=F32).astype(BF16)
    local[0].wait()
    local[1].wait()

    def src_z(d, k):
        return (z + nz - k) % nz if d == 0 else (z + k) % nz

    def off(d, k):
        return (nz - k) % nz if d == 0 else k % nz

    def dirs(k):
        return (0,) if (isinstance(k, int) and k in (0, nh)) else (0, 1)

    kcols = nz * ps

    def mix_block(b):
        side, j = b // (2 * NX), b % 2
        xs = (b // 2) % NX
        vv = lax.broadcasted_iota(jnp.int32, (ntb, kcols), 0)
        cc = lax.broadcasted_iota(jnp.int32, (ntb, kcols), 1)
        spread = (vv == 2 * ((cc // ps) * NX + xs) + j).astype(F32).astype(BF16)
        full = jnp.dot(lm[side], spread, preferred_element_type=F32)
        rr = lax.broadcasted_iota(jnp.int32, (mrows, kcols), 0) % ps
        qq = lax.broadcasted_iota(jnp.int32, (mrows, kcols), 1) % ps
        km[b] = jnp.where(rr == qq, full, 0.0).astype(BF16)

    per_step = -(-4 * NX // nh)

    def ladder_terms(s):
        total = acc[...]
        for xs in range(NX):
            base = 2 * (s * NX + xs)
            w = jnp.concatenate(
                [
                    jnp.concatenate([iv[idx[i, base]], iv[idx[i, base + 1]]], axis=1)
                    for i in range(2)
                ],
                axis=0,
            )
            block = jnp.concatenate([ga[s, xs], gb[s, xs]], axis=0)
            total = total + nt_dot(block, w)
        acc[...] = total

    def hop_a(k, j, last, ended):
        for d in range(2):
            s = src_z(d, k)
            if ended and j not in final[d]:
                continue
            ref = ga.at[s, parts[j]]
            rc(ref, ref, za_s.at[d, k, j], za_r.at[d, k, j], dev_z[d]).wait_recv()
            if not ended and (not last or j in final[d]):
                send_a(d, s, j, k + 1)

    def step(k):
        inner = not isinstance(k, int)

        def within(v, low, high):
            return inner or low <= v <= high

        if within(k, 1, nh - 1):
            for d in range(2):
                s = src_z(d, k)
                ref = gb.at[s, x]
                rc(ref, ref, zb_s.at[d, k], zb_r.at[d, k], dev_z[d]).wait_recv()
                if not inner and k == nh - 1:
                    ref = gb.at[s, x, half_b(d), :]
                rc(ref, ref, zb_s.at[d, k + 1], zb_r.at[d, k + 1], dev_z[d]).start()
        elif k == nh:
            s = src_z(0, nh)
            for d in range(2):
                ref = gb.at[s, x, half_b(d), :]
                rc(ref, ref, zb_s.at[d, nh], zb_r.at[d, nh], dev_z[d]).wait_recv()
        if within(k, 1, nh):
            for side in dirs(k):
                s, o = src_z(side, k), off(side, k)
                for d in range(2):
                    ref = gb.at[s, x]
                    rc(ref, ref, xb_s.at[o, d], xb_r.at[o, d], dev_x[d]).start()
        kx = k - X_LAG
        if within(kx, 0, nh):
            for side in dirs(kx):
                s, o = src_z(side, kx), off(side, kx)
                for d in range(2):
                    ref = gb.at[s, xfrom(d)]
                    rc(ref, ref, xb_s.at[o, d], xb_r.at[o, d], dev_x[d]).wait_recv()
                    ref = gb.at[s, xfrom(d), half_b(d), :]
                    rc(ref, ref, xb_s.at[o, 2 + d], xb_r.at[o, 2 + d], dev_x[d]).start()
        ka = k - A_LAG
        if within(ka, 1, nh):
            for j in range(3):
                hop_a(ka, j, not inner and ka == nh - 1, not inner and ka == nh)
        ko = k - 1
        if not inner and ko == 0:
            for d in range(2):
                ref = ga.at[z, xo, half_a(d), :]
                rc(ref, ref, xa_s.at[2 + d], xa_r.at[2 + d], dev_x[d]).wait_recv()
            for d in range(2):
                send_a(d, z, 3, 1)
        elif within(ko, 1, nh):
            hop_a(ko, 3, not inner and ko == nh - 1, not inner and ko == nh)
        if within(k, 1, nh):
            @pl.loop(0, per_step)
            def _(i):
                b = (k - 1) * per_step + i
                mix_block(b)
        kl = k - X_LAG - 1
        if not inner and kl == 0:
            for c in local[5:]:
                c.wait()
        if within(kl, 0, nh):
            for side in dirs(kl):
                s, o = src_z(side, kl), off(side, kl)
                for d in range(2):
                    ref = gb.at[s, xo, half_b(d), :]
                    rc(ref, ref, xb_s.at[o, 2 + d], xb_r.at[o, 2 + d], dev_x[d]).wait_recv()
                ladder_terms(s)

    ends = nh + X_LAG + 2
    begin = min(X_LAG + 2, ends)
    stop = max(begin, nh - 1)
    for k in range(1, begin):
        step(k)
    if stop > begin:
        @pl.loop(begin, stop)
        def _(k):
            step(k)
    for k in range(stop, ends):
        step(k)

    local[2].wait()
    ds[...] = (av[...].astype(F32) + acc[...]).astype(BF16)

    def order(i):
        return nh + (1 - 2 * (i % 2)) * ((i + 1) // 2)

    def rows_of(zz):
        return pl.ds(pl.multiple_of(zz * ps, ps), ps)

    def z_dev(o):
        return (z + o) % nz, {"tile": ((z + o) % nz) * NX + x}

    @pl.loop(0, nz - 1)
    def _(i):
        o = order(i)
        zz, dev = z_dev(o)
        rc(ds.at[rows_of(zz), :], e.at[0, x, z], zd_s.at[o], zd_r.at[o], dev).start()

    mine = pltpu.make_async_copy(ds.at[rows_of(z), :], e.at[0, x, z], loc.at[0])
    mine.start()
    mine.wait()

    def x_pass(o):
        zs = (z + nz - o) % nz
        for d in range(2):
            ref = e.at[0, x, zs]
            rc(ref, ref, xe_s.at[o, d], xe_r.at[o, d], dev_x[d]).start()

    def x_forward(o):
        zs = (z + nz - o) % nz
        for d in range(2):
            ref = e.at[0, xfrom(d), zs]
            rc(ref, ref, xe_s.at[o, d], xe_r.at[o, d], dev_x[d]).wait_recv()
        sgn = 1 - 2 * (o % 2)
        ref = e.at[0, (x + NX - sgn) % NX, zs]
        dev = {"tile": z * NX + (x + NX + sgn) % NX}
        rc(ref, ref, xe_s.at[o, 2], xe_r.at[o, 2], dev).start()

    x_pass(0)

    @pl.loop(0, nz - 1)
    def _(i):
        o = order(nz - 2 - i)
        zs = (z + nz - o) % nz
        ref = e.at[0, x, zs]
        rc(ref, ref, zd_s.at[o], zd_r.at[o], {"tile": zs * NX + x}).wait_recv()
        x_pass(o)

    def to_partner(dx):
        xs = (x + dx) % NX
        rc(e.at[0, xs], e.at[1, xs], pe_s.at[dx], pe_r.at[dx], dev_p).start()

    def mix(side, dx):
        xs = (x + dx) % NX
        for j in range(2):
            rhs = e[side, xs, :, :, j * tw : (j + 1) * tw].reshape(kcols, tw)
            b = (side * NX + xs) * 2 + j
            acc2[...] += jnp.dot(km[b], rhs, preferred_element_type=F32)

    to_partner(0)
    x_forward(0)

    @pl.loop(0, nz - 1)
    def _(i):
        x_forward(order(nz - 2 - i))

    to_partner(1)
    to_partner(3)
    acc2[...] = jnp.zeros_like(acc2)
    mix(0, 0)
    mix(0, 1)
    mix(0, 3)

    @pl.loop(0, nz)
    def _(o):
        zs = (z + nz - o) % nz
        ref = e.at[0, xo, zs]
        rc(ref, ref, xe_s.at[o, 2], xe_r.at[o, 2], dev_x[0]).wait_recv()

    to_partner(2)
    mix(0, 2)
    for dx in (0, 1, 3, 2):
        xs = (x + dx) % NX
        rc(e.at[0, xs], e.at[1, xs], pe_s.at[dx], pe_r.at[dx], dev_p).wait_recv()
        mix(1, dx)

    rs[...] = acc2[...].astype(BF16).reshape(rs.shape)

    @pl.loop(0, nz - 1)
    def _(i):
        o = order(i)
        zz, dev = z_dev(o)
        rc(rs.at[zz], r.at[z], zr_s.at[o], zr_r.at[o], dev).start()

    r[z] = rs[z]

    def sent(ref, sem):
        rc(ref, ref, sem, sem, dev_p).wait_send()

    for d in range(2):
        sent(own_a, xa_s.at[d])
        sent(ga.at[z, x, half_a(d), :], xa_s.at[2 + d])

        @pl.loop(1, nh)
        def _(k):
            sent(own_b, zb_s.at[d, k])
            for j in range(NX):
                sent(own_a, za_s.at[d, k, j])

        sent(gb.at[z, x, half_b(d), :], zb_s.at[d, nh])
        for j in final[d]:
            sent(own_a, za_s.at[d, nh, j])

    @pl.loop(0, nz)
    def _(o):
        for d in range(2):
            sent(gb.at[z, x], xb_s.at[o, d])
            sent(gb.at[z, x, half_b(d), :], xb_s.at[o, 2 + d])
            sent(e.at[0, x, z], xe_s.at[o, d])
        sent(e.at[0, x, z], xe_s.at[o, 2])

    for dx in range(NX):
        sent(e.at[0, 0], pe_s.at[dx])

    @pl.loop(1, nz)
    def _(o):
        zs = (z + nz - o) % nz
        rc(r.at[zs], r.at[zs], zr_s.at[o], zr_r.at[o], {"tile": zs * NX + x}).wait_recv()
        sent(e.at[0, x, z], zd_s.at[o])
        sent(rs.at[z], zr_s.at[o])

    for j in range(2):
        back = r[:, j].reshape(pairs, tw).astype(F32)
        lanes = slice(j * tw, (j + 1) * tw)
        out[:, lanes] = (acc[:, lanes] + back).astype(BF16)


def on_device(amplitudes, slot_cols, slot_count, integrals, cycle_same, cycle_cross):
    pairs, width = amplitudes.shape
    rows, slots, tw, _ = integrals.shape
    ntb = cycle_same.shape[1]
    nz = lax.axis_size("tile") // NX
    ps = pairs // nz
    ra = (3 * pairs // 8) // 32 * 32
    rb = pairs - ra
    nh = nz // 2
    live = lax.broadcasted_iota(jnp.int32, (rows, slots), 1) < slot_count[:, None]
    cols = jnp.where(live, slot_cols, ntb)
    hit = cols[:, :, None] == lax.broadcasted_iota(jnp.int32, (rows, slots, ntb), 2)
    number = lax.broadcasted_iota(jnp.int32, (rows, slots, ntb), 0) * slots
    number = number + lax.broadcasted_iota(jnp.int32, (rows, slots, ntb), 1)
    idx = jnp.min(jnp.where(hit, number, rows * slots), axis=1)

    dma = pltpu.SemaphoreType.DMA
    anyspace = pl.BlockSpec(memory_space=pl.ANY)
    vm = pltpu.VMEM
    mrows = nz * 2 * ps
    nb = 4 * NX
    per_step = -(-nb // nh)
    return pl.pallas_call(
        functools.partial(kernel, nz, ra),
        out_shape=jax.ShapeDtypeStruct((pairs, width), BF16),
        in_specs=[pl.BlockSpec(memory_space=pltpu.SMEM)] + [anyspace] * 4,
        out_specs=pl.BlockSpec(memory_space=pltpu.VMEM),
        scratch_shapes=[
            vm((nz, NX, ra, width), BF16),
            vm((nz, NX, rb, width), BF16),
            vm((rows * slots + 1, tw, tw), BF16),
            vm((2, ntb, ntb), BF16),
            vm((2, mrows, ntb), BF16),
            vm((per_step * nh, mrows, nz * ps), BF16),
            vm((pairs, width), BF16),
            vm((pairs, width), F32),
            vm((mrows, tw), F32),
            vm((pairs, width), BF16),
            vm((2, NX, nz, ps, width), BF16),
            vm((nz, 2, ps, tw), BF16),
            vm((nz, 2, ps, tw), BF16),
            dma((7,)),
            dma((2, nh + 1)), dma((2, nh + 1)),
            dma((2, nh + 1, NX)), dma((2, nh + 1, NX)),
            dma((4,)), dma((4,)),
            dma((nz, 4)), dma((nz, 4)),
            dma((nz,)), dma((nz,)),
            dma((nz, 3)), dma((nz, 3)),
            dma((NX,)), dma((NX,)),
            dma((nz,)), dma((nz,)),
        ],
        compiler_params=pltpu.CompilerParams(
            collective_id=0, has_side_effects=True, vmem_limit_bytes=67043328
        ),
    )(idx, amplitudes, integrals, cycle_same, cycle_cross)


def solution(mesh):
    in_specs = (
        P(None, ("sym", "tile")),
        P(("sym", "tile"), None),
        P(("sym", "tile")),
        P(("sym", "tile"), None, None, None),
        P("sym", None, None),
        P("sym", None, None),
    )
    return jax.shard_map(
        on_device, mesh=mesh, in_specs=in_specs, out_specs=P(None, ("sym", "tile")), check_vma=False
    )
```
